32 devices in a mesh: cp: 8 (over z, x), tp: 4 (over y, core).
Axes of the slice: x: 2, y: 2, z: 4, core: 2. Of those that a mesh axis runs over, the one named last changes fastest.
Arguments:
- queries: bfloat16 [1536, 2048], P('cp', 'tp'), may hold values from -128 to 128
- keys: bfloat16 [1536, 256], P('cp'), may hold values from -6 to 6
- values: bfloat16 [1536, 256], P('cp'), may hold values from -6 to 6
- positions: int32 [1536], replicated, may hold values from 0 to 1535, as said below
- out_weight: bfloat16 [2048, 8192], P('tp'), may hold values from -0.125 to 0.125
Outputs:
- mixed: bfloat16 [1536, 8192], P(('cp', 'tp'))
The draws below stay inside these ranges and needn't reach their ends.
Inputs may be any that keep to these rules, and one draw needn't show every extreme that they name: positions is a permutation of 0 to 1535. The tokens stored at indices d * 192 to (d + 1) * 192 - 1 form two runs of 96 consecutive positions, the first starting at b * 96 and the second at (15 - b) * 96 for some b, each b used by one d.
All inputs are finite; a program needn't handle non-finite values.
Results may differ from the reference program's by a relative error of at most 0.013.
Values may be sent and summed in bfloat16 or wider, within the bound.
No kernel may reach another device: no remote copies, remote signals or barrier semaphores. Data moves between devices by JAX's collectives and lax.ppermute only.
A program may use at most 128 MiB of HBM per device.

```python
import math
import jax
import jax.numpy as jnp
from jax import lax

D = 8192
HEAD = 128
GROUP = 8
KV = 2
TOK_DEV = 192
H = 16
TOKENS = 1536
N_TP = 4


def joint_draw(key):
    seed_base = jax.random.fold_in(key, 11)
    seed_query, seed_keys = jax.random.split(seed_base, 2)
    queries = jnp.clip(jax.random.normal(seed_query, (TOKENS, GROUP * KV * HEAD), jnp.float32), -6.0, 6.0)
    keys = jnp.clip(jax.random.normal(seed_keys, (TOKENS, KV * HEAD), jnp.float32), -6.0, 6.0)
    return (queries, keys)


def draw_queries(key, part):
    return joint_draw(key)[0].astype(jnp.bfloat16)


def draw_keys(key, part):
    return joint_draw(key)[1].astype(jnp.bfloat16)


def draw_positions(key, part):
    slot_count = TOKENS // TOK_DEV
    half_rows = TOK_DEV // 2
    slot_order = jax.random.permutation(jax.random.fold_in(key, 5), slot_count)
    block_start = jnp.stack([slot_order, 2 * slot_count - 1 - slot_order], axis=1)
    position = block_start[:, :, None] * half_rows + jnp.arange(half_rows)[None, None, :]
    return position.reshape(-1).astype(jnp.int32)


def block_levels(own_key, extent, shards, smallest, top_value):
    gain, own = 1.0, jax.random.fold_in(own_key, 6)
    for axis_at, parts in shards:
        heights = jnp.exp(jax.random.uniform(jax.random.fold_in(own, axis_at), (parts,), jnp.float32, smallest / len(shards), top_value / len(shards)))
        gain = gain * jnp.repeat(heights, extent[axis_at] // parts).reshape([-1 if axis == axis_at else 1 for axis in range(len(extent))])
    return gain


def bell_draw(own_key, extent, spread, most, cuts=(), kind=jnp.bfloat16):
    level = block_levels(own_key, extent, cuts, -0.22, 0.18) if cuts else 1.0
    entries = jax.random.normal(own_key, extent, jnp.float32) * spread * level
    return jnp.minimum(jnp.maximum(entries, -most), most).astype(kind)


def setup_inputs(seed: int = 0) -> dict:
    splits = jax.random.split(jax.random.key(seed), 6)
    queries = draw_queries(jax.random.fold_in(splits[5], 71), 0)
    keys = draw_keys(jax.random.fold_in(splits[5], 71), 0)
    values = bell_draw(splits[2], (TOKENS, KV * HEAD), 1.0, 6.0, ((0, 8),))
    positions = draw_positions(jax.random.fold_in(splits[5], 71), 0)
    out_weight = bell_draw(splits[4], (H * HEAD, D), (H * HEAD) ** -0.5, 0.125, ((0, 4),))
    return dict(queries=queries, keys=keys, values=values, positions=positions, out_weight=out_weight)


def reference(queries, keys, values, positions, out_weight):
    token_count = queries.shape[0]
    head_count = queries.shape[1] // HEAD
    score_scale = HEAD ** -0.5
    block_rows = math.gcd(token_count, 512)

    def one_block(block_index):
        first = (block_index * block_rows).astype(jnp.int32)
        query_block = lax.dynamic_slice_in_dim(queries, first, block_rows, 0)
        query_pos = lax.dynamic_slice_in_dim(positions, first, block_rows, 0)
        allowed = positions[None, :] <= query_pos[:, None]

        def one_head(head_index):
            kv_group = head_index // GROUP
            query_head = lax.dynamic_slice_in_dim(query_block, (head_index * HEAD).astype(jnp.int32), HEAD, 1)
            key_head = lax.dynamic_slice_in_dim(keys, (kv_group * HEAD).astype(jnp.int32), HEAD, 1)
            value_head = lax.dynamic_slice_in_dim(values, (kv_group * HEAD).astype(jnp.int32), HEAD, 1)
            scores = jnp.dot(query_head, key_head.T, preferred_element_type=jnp.float32) * score_scale
            scores = jnp.where(allowed, scores, -1e30)
            row_max = jnp.max(scores, axis=1, keepdims=True)
            weights = jnp.where(allowed, jnp.exp(scores - row_max), 0.0)
            row_sum = jnp.sum(weights, axis=1, keepdims=True)
            head_out = jnp.dot(weights.astype(jnp.bfloat16), value_head, preferred_element_type=jnp.float32) / row_sum
            return head_out.astype(jnp.bfloat16)

        stacked = lax.map(one_head, jnp.arange(head_count, dtype=jnp.int32))
        return jnp.transpose(stacked, (1, 0, 2)).reshape(block_rows, head_count * HEAD)

    attended = lax.map(one_block, jnp.arange(token_count // block_rows, dtype=jnp.int32))
    attended = attended.reshape(token_count, head_count * HEAD)
    slab_width = attended.shape[1] // N_TP
    mixed = jnp.zeros((token_count, out_weight.shape[1]), jnp.float32)
    for slab in range(N_TP):
        partial_sum = jnp.dot(attended[:, slab * slab_width:(slab + 1) * slab_width],
                              out_weight[slab * slab_width:(slab + 1) * slab_width],
                              preferred_element_type=jnp.float32).astype(jnp.bfloat16)
        partial_sum = lax.optimization_barrier(partial_sum)
        mixed = mixed + partial_sum.astype(jnp.float32)
    return mixed.astype(jnp.bfloat16)
```

```python
import functools

import jax
import jax.numpy as jnp
from jax import lax
from jax.experimental import pallas as pl
from jax.experimental.pallas import tpu as pltpu
from jax.sharding import PartitionSpec as P

HEAD = 128
GROUP = 8
NEG = -1e30
LOG2E = 1.4426950408889634
AXES = ("cp", "tp")
COLUMN_CUTS = (0, 2, 8, 16)


def attention_kernel(*refs):
    bias_ref, own_ref, sib_ref = refs[:3]
    block_refs = refs[3:-2]
    outs = refs[-2:]
    keys = jnp.concatenate([r[:, :HEAD] for r in block_refs], axis=0)
    values = jnp.concatenate([r[:, HEAD:] for r in block_refs], axis=0)
    scale = HEAD ** (-0.5) * LOG2E
    for q_ref, out_ref in zip((own_ref, sib_ref), outs):
        for head in range(q_ref.shape[1] // HEAD):
            cols = slice(head * HEAD, (head + 1) * HEAD)
            scores = lax.dot_general(
                q_ref[:, cols], keys, (((1,), (1,)), ((), ())), preferred_element_type=jnp.float32
            )
            scores = scores + bias_ref[...]
            top = jnp.max(scores, axis=1, keepdims=True)
            weights = jnp.exp2((scores - top) * scale)
            total = jnp.sum(weights, axis=1, keepdims=True)
            mixed = jnp.dot(
                weights.astype(jnp.bfloat16), values, preferred_element_type=jnp.float32
            )
            out_ref[:, cols] = (mixed / total).astype(jnp.bfloat16)


def pairing(cp_size):
    low = [o for o in range(2, cp_size) if o < cp_size // 2]
    high = [o for o in range(2, cp_size) if o >= cp_size // 2]
    high = sorted(high, key=lambda o: (o & 1, -o))
    order = high + low
    return [(order[i], order[i + 1]) for i in range(0, len(order), 2)]


def shards(cp_size, tp_size, queries, keys, values, positions, out_weight):
    rows = queries.shape[0]
    heads = queries.shape[1] // HEAD
    part = rows // tp_size
    cp = lax.axis_index("cp")
    tp = lax.axis_index("tp")
    core = tp % 2

    def permute(x, to_cp, to_tp):
        pairs = [
            (c * tp_size + t, to_cp(c, t) * tp_size + to_tp(t))
            for c in range(cp_size)
            for t in range(tp_size)
        ]
        return lax.ppermute(x, AXES, pairs)

    def to_sibling(x):
        return permute(x, lambda c, t: c, lambda t: t ^ 1)

    kv_group = tp * heads // GROUP
    block = jnp.concatenate(
        [lax.dynamic_slice_in_dim(a, kv_group * HEAD, HEAD, 1) for a in (keys, values)], axis=1
    )
    blocks = [block]
    offsets = [(0, 0)]
    fetched = []
    for pair in pairing(cp_size):
        got = permute(block, lambda c, t, pair=pair: c ^ pair[t & 1], lambda t: t)
        fetched.append(got)
        blocks.append(got)
        offsets.append(pair)
    blocks.append(permute(block, lambda c, t: c ^ 1, lambda t: t))
    offsets.append((1, 1))
    for got, pair in zip(fetched, pairing(cp_size)):
        blocks.append(to_sibling(got))
        offsets.append((pair[1], pair[0]))

    def rows_of(x, c):
        return jnp.concatenate(
            [
                lax.dynamic_slice_in_dim(x, ((tp // 2 + s) % 2 * 2 + c) * part, part, 0)
                for s in (0, 1)
            ],
            axis=0,
        )

    own_q = rows_of(queries, core)
    sib_q = to_sibling(rows_of(queries, 1 - core))
    sib_weight = to_sibling(out_weight)

    query_pos = rows_of(lax.dynamic_slice_in_dim(positions, cp * rows, rows, 0), core)
    key_pos = jnp.concatenate(
        [
            lax.dynamic_slice_in_dim(positions, (cp ^ jnp.where(core == 0, a, b)) * rows, rows, 0)
            for a, b in offsets
        ]
    )
    bias = jnp.where(key_pos[None, :] <= query_pos[:, None], 0.0, NEG).astype(jnp.float32)

    attended = jax.ShapeDtypeStruct(own_q.shape, jnp.bfloat16)
    own_a, sib_a = pl.pallas_call(
        attention_kernel,
        out_shape=(attended, attended),
        name="attention",
    )(bias, own_q, sib_q, *blocks)

    width = out_weight.shape[1]
    outs = []
    for lo, hi in zip(COLUMN_CUTS[:-1], COLUMN_CUTS[1:]):
        cols = slice(lo * width // COLUMN_CUTS[-1], hi * width // COLUMN_CUTS[-1])
        partial = (
            jnp.dot(own_a, out_weight[:, cols], preferred_element_type=jnp.float32)
            + jnp.dot(sib_a, sib_weight[:, cols], preferred_element_type=jnp.float32)
        ).astype(jnp.bfloat16)
        got = permute(partial[part:], lambda c, t: c, lambda t: t ^ 2)
        outs.append(
            (partial[:part].astype(jnp.float32) + got.astype(jnp.float32)).astype(jnp.bfloat16)
        )
    return jnp.concatenate(outs, axis=1)


def solution(mesh):
    in_specs = (P("cp", "tp"), P("cp", None), P("cp", None), P(), P("tp", None))
    out_specs = P(("cp", "tp"), None)
    body = functools.partial(shards, mesh.shape["cp"], mesh.shape["tp"])
    return jax.shard_map(body, mesh=mesh, in_specs=in_specs, out_specs=out_specs, check_vma=False)
```

```python
import functools

import jax
import jax.numpy as jnp
from jax import lax
from jax.experimental import pallas as pl
from jax.experimental.pallas import tpu as pltpu
from jax.sharding import PartitionSpec as P

HEAD = 128
GROUP = 8
NEG = -1e30
LOG2E = 1.4426950408889634
AXES = ("cp", "tp")
VMEM_LIMIT = 36 * 2**20
COLUMN_CUTS = (0, 4, 10, 16)
TILE = 512


def project(attended, weight, keep_ref, send_ref):
    partial = jnp.dot(attended, weight, preferred_element_type=jnp.float32).astype(jnp.bfloat16)
    part = keep_ref.shape[0]
    keep_ref[...] = partial[:part]
    send_ref[...] = partial[part:]


def attention_kernel(stack, *refs):
    bias_ref, own_ref, sib_ref, own_w_ref, sib_w_ref = refs[:5]
    block_refs = refs[5:-5]
    attended_ref, keep_ref, send_ref, weight_ref, sems = refs[-5:]
    half, width = own_w_ref.shape[0], weight_ref.shape[1]
    loads = [
        pltpu.make_async_copy(
            ref.at[:, pl.ds(0, width)], weight_ref.at[pl.ds(i * half, half)], sems.at[i]
        )
        for i, ref in enumerate((own_w_ref, sib_w_ref))
    ]
    for load in loads:
        load.start()
    keys = jnp.concatenate([r[:, :HEAD] for r in block_refs], axis=0)
    values = jnp.concatenate([r[:, HEAD:] for r in block_refs], axis=0)
    values = jnp.concatenate([values, jnp.ones_like(values)], axis=1)
    scale = HEAD ** (-0.5) * LOG2E
    rows = own_ref.shape[0]
    heads = own_ref.shape[1] // HEAD
    for side, q_ref in enumerate((own_ref, sib_ref)):
        for first in range(0, heads, stack):
            q = jnp.concatenate(
                [q_ref[:, h * HEAD : (h + 1) * HEAD] for h in range(first, first + stack)], axis=0
            )
            scores = lax.dot_general(
                q, keys, (((1,), (1,)), ((), ())), preferred_element_type=jnp.float32
            )
            scores = (scores.reshape(stack, rows, -1) + bias_ref[...][None]).reshape(scores.shape)
            top = jnp.max(scores, axis=1, keepdims=True)
            weights = jnp.exp2((scores - top) * scale).astype(jnp.bfloat16)
            mixed = jnp.dot(weights, values, preferred_element_type=jnp.float32)
            result = (mixed[:, :HEAD] / mixed[:, HEAD:]).astype(jnp.bfloat16)
            for i in range(stack):
                at = (side * heads + first + i) * HEAD
                attended_ref[:, at : at + HEAD] = result[i * rows : (i + 1) * rows]
    for load in loads:
        load.wait()
    project(attended_ref[...], weight_ref[...], keep_ref, send_ref)


def project_kernel(attended_ref, own_w_ref, sib_w_ref, keep_ref, send_ref):
    weight = jnp.concatenate([own_w_ref[...], sib_w_ref[...]], axis=0)
    project(attended_ref[...], weight, keep_ref, send_ref)


def pairing(cp_size):
    low = [o for o in range(2, cp_size) if o < cp_size // 2]
    high = [o for o in range(2, cp_size) if o >= cp_size // 2]
    high = sorted(high, key=lambda o: (o & 1, -o))
    order = high + low
    return [(order[i], order[i + 1]) for i in range(0, len(order), 2)]


def shards(cp_size, tp_size, queries, keys, values, positions, out_weight):
    rows = queries.shape[0]
    heads = queries.shape[1] // HEAD
    part = rows // tp_size
    cp = lax.axis_index("cp")
    tp = lax.axis_index("tp")
    core = tp % 2

    def permute(x, to_cp, to_tp):
        pairs = [
            (c * tp_size + t, to_cp(c, t) * tp_size + to_tp(t))
            for c in range(cp_size)
            for t in range(tp_size)
        ]
        return lax.ppermute(x, AXES, pairs)

    def to_sibling(x):
        return permute(x, lambda c, t: c, lambda t: t ^ 1)

    kv_group = tp * heads // GROUP
    block = jnp.concatenate(
        [lax.dynamic_slice_in_dim(a, kv_group * HEAD, HEAD, 1) for a in (keys, values)], axis=1
    )
    blocks = [block]
    offsets = [(0, 0)]
    fetched = []
    for pair in pairing(cp_size):
        got = permute(block, lambda c, t, pair=pair: c ^ pair[t & 1], lambda t: t)
        fetched.append(got)
        blocks.append(got)
        offsets.append(pair)
    blocks.append(permute(block, lambda c, t: c ^ 1, lambda t: t))
    offsets.append((1, 1))
    for got, pair in zip(fetched, pairing(cp_size)):
        blocks.append(to_sibling(got))
        offsets.append((pair[1], pair[0]))

    def rows_of(x, c):
        return jnp.concatenate(
            [
                lax.dynamic_slice_in_dim(x, ((tp // 2 + s) % 2 * 2 + c) * part, part, 0)
                for s in (0, 1)
            ],
            axis=0,
        )

    own_q = rows_of(queries, core)
    sib_q = to_sibling(rows_of(queries, 1 - core))
    sib_weight = to_sibling(out_weight)

    query_pos = rows_of(lax.dynamic_slice_in_dim(positions, cp * rows, rows, 0), core)
    key_pos = jnp.concatenate(
        [
            lax.dynamic_slice_in_dim(positions, (cp ^ jnp.where(core == 0, a, b)) * rows, rows, 0)
            for a, b in offsets
        ]
    )
    bias = jnp.where(key_pos[None, :] <= query_pos[:, None], 0.0, NEG).astype(jnp.float32)

    width = out_weight.shape[1]
    cuts = [c * width // COLUMN_CUTS[-1] for c in COLUMN_CUTS]
    vmem = functools.partial(pltpu.with_memory_space_constraint, memory_space=pltpu.VMEM)
    hbm = pl.BlockSpec(memory_space=pltpu.HBM)
    weights = [pltpu.with_memory_space_constraint(w, pltpu.HBM) for w in (out_weight, sib_weight)]
    whole = pl.BlockSpec(memory_space=pltpu.VMEM)
    attended = None
    outs = []
    for lo, hi in zip(cuts[:-1], cuts[1:]):
        half = pltpu.VMEM((part, hi - lo), jnp.bfloat16)
        if attended is None:
            stack = min(heads, max(1, 4 * 1536 // bias.shape[1]))
            attended, keep, send = pl.pallas_call(
                functools.partial(attention_kernel, stack),
                in_specs=[whole] * 3 + [hbm] * 2 + [whole] * len(blocks),
                out_shape=(pltpu.VMEM((2 * part, 2 * heads * HEAD), jnp.bfloat16), half, half),
                scratch_shapes=[
                    pltpu.VMEM((2 * heads * HEAD, hi - lo), jnp.bfloat16),
                    pltpu.SemaphoreType.DMA((2,)),
                ],
                compiler_params=pltpu.CompilerParams(vmem_limit_bytes=VMEM_LIMIT),
                name="attention",
            )(vmem(bias), vmem(own_q), vmem(sib_q), *weights, *[vmem(b) for b in blocks])
        else:
            tile = pl.BlockSpec((heads * HEAD, TILE), lambda i, lo=lo: (0, lo // TILE + i))
            side = pl.BlockSpec((part, TILE), lambda i: (0, i))
            keep, send = pl.pallas_call(
                project_kernel,
                grid=((hi - lo) // TILE,),
                in_specs=[whole, tile, tile],
                out_specs=(side, side),
                out_shape=(half, half),
                compiler_params=pltpu.CompilerParams(vmem_limit_bytes=VMEM_LIMIT),
                name="project",
            )(attended, *weights)
        got = permute(send, lambda c, t: c, lambda t: t ^ 2)
        outs.append((keep.astype(jnp.float32) + got.astype(jnp.float32)).astype(jnp.bfloat16))
    return jnp.concatenate(outs, axis=1)


def solution(mesh):
    in_specs = (P("cp", "tp"), P("cp", None), P("cp", None), P(), P("tp", None))
    out_specs = P(("cp", "tp"), None)
    body = functools.partial(shards, mesh.shape["cp"], mesh.shape["tp"])
    return jax.shard_map(body, mesh=mesh, in_specs=in_specs, out_specs=out_specs, check_vma=False)
```

```python
import functools

import jax
import jax.numpy as jnp
from jax import lax
from jax.experimental import pallas as pl
from jax.experimental.pallas import tpu as pltpu
from jax.sharding import PartitionSpec as P


HEAD = 128
GROUP = 8
NEG = -1e30
LOG2E = 1.4426950408889634
AXES = ("cp", "tp")
VMEM_LIMIT = 36 * 2**20
COLUMN_CUTS = (0, 4, 10, 16)
TILE = 512


def project(attended, weight, keep_ref, send_ref):
    partial = jnp.dot(attended, weight, preferred_element_type=jnp.float32).astype(jnp.bfloat16)
    part = keep_ref.shape[0]
    keep_ref[...] = partial[:part]
    send_ref[...] = partial[part:]


def attention_kernel(stack, *refs):
    bias_ref, own_ref, sib_ref, own_w_ref, sib_w_ref = refs[:5]
    block_refs = refs[5:-5]
    attended_ref, keep_ref, send_ref, weight_ref, sems = refs[-5:]
    half, width = own_w_ref.shape[0], weight_ref.shape[1]
    loads = [
        pltpu.make_async_copy(
            ref.at[:, pl.ds(0, width)], weight_ref.at[pl.ds(i * half, half)], sems.at[i]
        )
        for i, ref in enumerate((own_w_ref, sib_w_ref))
    ]
    for load in loads:
        load.start()

    @pl.when(bias_ref[0, 0] <= 0.0)
    def _():
        keys = jnp.concatenate([r[:, :HEAD] for r in block_refs], axis=0)
        values = jnp.concatenate([r[:, HEAD:] for r in block_refs], axis=0)
        values = jnp.concatenate([values, jnp.ones_like(values)], axis=1)
        scale = HEAD ** (-0.5) * LOG2E
        rows = own_ref.shape[0]
        heads = own_ref.shape[1] // HEAD
        for side, q_ref in enumerate((own_ref, sib_ref)):
            for first in range(0, heads, stack):
                q = jnp.concatenate(
                    [q_ref[:, h * HEAD : (h + 1) * HEAD] for h in range(first, first + stack)], axis=0
                )
                scores = lax.dot_general(
                    q, keys, (((1,), (1,)), ((), ())), preferred_element_type=jnp.float32
                )
                scores = (scores.reshape(stack, rows, -1) + bias_ref[...][None]).reshape(scores.shape)
                top = jnp.max(scores, axis=1, keepdims=True)
                weights = jnp.exp2((scores - top) * scale).astype(jnp.bfloat16)
                mixed = jnp.dot(weights, values, preferred_element_type=jnp.float32)
                result = (mixed[:, :HEAD] / mixed[:, HEAD:]).astype(jnp.bfloat16)
                for i in range(stack):
                    at = (side * heads + first + i) * HEAD
                    attended_ref[:, at : at + HEAD] = result[i * rows : (i + 1) * rows]

    for load in loads:
        load.wait()
    project(attended_ref[...], weight_ref[...], keep_ref, send_ref)


def project_kernel(first, attended_ref, own_w_ref, sib_w_ref, keep_ref, send_ref, weight_ref, sems):
    half = own_w_ref.shape[0]
    tiles, _, tile = weight_ref.shape
    loads = [
        [
            pltpu.make_async_copy(
                ref.at[:, pl.ds(first + t * tile, tile)],
                weight_ref.at[t, pl.ds(i * half, half)],
                sems.at[t, i],
            )
            for i, ref in enumerate((own_w_ref, sib_w_ref))
        ]
        for t in range(tiles)
    ]
    for pair in loads:
        for load in pair:
            load.start()
    for t, pair in enumerate(loads):
        for load in pair:
            load.wait()
        cols = pl.ds(t * tile, tile)
        project(attended_ref[...], weight_ref[t], keep_ref.at[:, cols], send_ref.at[:, cols])


def finish_kernel(first, *refs):
    keep_ref, got_ref = refs[:2]
    out_ref, sum_ref, sem = refs[-3:]
    sum_ref[...] = (
        keep_ref[...].astype(jnp.float32) + got_ref[...].astype(jnp.float32)
    ).astype(jnp.bfloat16)
    store = pltpu.make_async_copy(
        sum_ref, out_ref.at[:, pl.ds(first, sum_ref.shape[1])], sem
    )
    store.start()
    store.wait()


def pairing(cp_size):
    low = [o for o in range(2, cp_size) if o < cp_size // 2]
    high = [o for o in range(2, cp_size) if o >= cp_size // 2]
    high = sorted(high, key=lambda o: (o & 1, -o))
    order = high + low
    return [(order[i], order[i + 1]) for i in range(0, len(order), 2)]


def shards(cp_size, tp_size, queries, keys, values, positions, out_weight):
    rows = queries.shape[0]
    heads = queries.shape[1] // HEAD
    part = rows // tp_size
    cp = lax.axis_index("cp")
    tp = lax.axis_index("tp")
    core = tp % 2

    def permute(x, to_cp, to_tp):
        pairs = [
            (c * tp_size + t, to_cp(c, t) * tp_size + to_tp(t))
            for c in range(cp_size)
            for t in range(tp_size)
        ]
        return lax.ppermute(x, AXES, pairs)

    def to_sibling(x):
        return permute(x, lambda c, t: c, lambda t: t ^ 1)

    kv_group = tp * heads // GROUP
    block = jnp.concatenate(
        [lax.dynamic_slice_in_dim(a, kv_group * HEAD, HEAD, 1) for a in (keys, values)], axis=1
    )
    blocks = [block]
    offsets = [(0, 0)]
    fetched = []
    for pair in pairing(cp_size):
        arrived = permute(block, lambda c, t, pair=pair: c ^ pair[t & 1], lambda t: t)
        fetched.append(arrived)
        blocks.append(arrived)
        offsets.append(pair)
    blocks.append(permute(block, lambda c, t: c ^ 1, lambda t: t))
    offsets.append((1, 1))
    for arrived, pair in zip(fetched, pairing(cp_size)):
        blocks.append(to_sibling(arrived))
        offsets.append((pair[1], pair[0]))

    def rows_of(x, c):
        return jnp.concatenate(
            [
                lax.dynamic_slice_in_dim(x, ((tp // 2 + s) % 2 * 2 + c) * part, part, 0)
                for s in (0, 1)
            ],
            axis=0,
        )

    own_q = rows_of(queries, core)
    sib_q = to_sibling(rows_of(queries, 1 - core))
    sib_weight = to_sibling(out_weight)

    query_pos = rows_of(lax.dynamic_slice_in_dim(positions, cp * rows, rows, 0), core)
    key_pos = jnp.concatenate(
        [
            lax.dynamic_slice_in_dim(positions, (cp ^ jnp.where(core == 0, a, b)) * rows, rows, 0)
            for a, b in offsets
        ]
    )
    bias = jnp.where(key_pos[None, :] <= query_pos[:, None], 0.0, NEG).astype(jnp.float32)

    width = out_weight.shape[1]
    cuts = [c * width // COLUMN_CUTS[-1] for c in COLUMN_CUTS]
    vmem = functools.partial(pltpu.with_memory_space_constraint, memory_space=pltpu.VMEM)
    hbm = pl.BlockSpec(memory_space=pltpu.HBM)
    weights = [pltpu.with_memory_space_constraint(w, pltpu.HBM) for w in (out_weight, sib_weight)]
    whole = pl.BlockSpec(memory_space=pltpu.VMEM)
    attended = None
    kept = []
    got = []
    for lo, hi in zip(cuts[:-1], cuts[1:]):
        half = pltpu.VMEM((part, hi - lo), jnp.bfloat16)
        if attended is None:
            stack = min(heads, max(1, 2 * 1536 // bias.shape[1]))
            attended, keep, send = pl.pallas_call(
                functools.partial(attention_kernel, stack),
                in_specs=[whole] * 3 + [hbm] * 2 + [whole] * len(blocks),
                out_shape=(pltpu.VMEM((2 * part, 2 * heads * HEAD), jnp.bfloat16), half, half),
                scratch_shapes=[
                    pltpu.VMEM((2 * heads * HEAD, hi - lo), jnp.bfloat16),
                    pltpu.SemaphoreType.DMA((2,)),
                ],
                compiler_params=pltpu.CompilerParams(vmem_limit_bytes=VMEM_LIMIT),
                name="attention",
            )(vmem(bias), vmem(own_q), vmem(sib_q), *weights, *[vmem(b) for b in blocks])
        else:
            keep, send = pl.pallas_call(
                functools.partial(project_kernel, lo),
                in_specs=[whole, hbm, hbm],
                out_shape=(half, half),
                scratch_shapes=[
                    pltpu.VMEM(((hi - lo) // TILE, 2 * heads * HEAD, TILE), jnp.bfloat16),
                    pltpu.SemaphoreType.DMA(((hi - lo) // TILE, 2)),
                ],
                compiler_params=pltpu.CompilerParams(vmem_limit_bytes=VMEM_LIMIT),
                name="project",
            )(attended, *weights)
        kept.append(keep)
        got.append(permute(send, lambda c, t: c, lambda t: t ^ 2))
    out = ()
    for lo, hi, keep, arrived in zip(cuts[:-1], cuts[1:], kept, got):
        out = pl.pallas_call(
            functools.partial(finish_kernel, lo),
            in_specs=[whole, whole] + [hbm] * len(out),
            out_specs=(hbm,),
            out_shape=(pltpu.HBM((part, width), jnp.bfloat16),),
            scratch_shapes=[pltpu.VMEM((part, hi - lo), jnp.bfloat16), pltpu.SemaphoreType.DMA],
            input_output_aliases={2: 0} if out else {},
            name="finish",
        )(vmem(keep), vmem(arrived), *out)
    return out[0]


def solution(mesh):
    in_specs = (P("cp", "tp"), P("cp", None), P("cp", None), P(), P("tp", None))
    out_specs = P(("cp", "tp"), None)
    cp_size, tp_size = mesh.shape["cp"], mesh.shape["tp"]

    def body(*args):
        return shards(cp_size, tp_size, *args)

    return jax.shard_map(body, mesh=mesh, in_specs=in_specs, out_specs=out_specs, check_vma=False)
```

```python
import functools

import jax
import jax.numpy as jnp
from jax import lax
from jax.experimental import pallas as pl
from jax.experimental.pallas import tpu as pltpu
from jax.sharding import PartitionSpec as P


HEAD = 128
GROUP = 8
NEG = -1e30
LOG2E = 1.4426950408889634
AXES = ("cp", "tp")
VMEM_LIMIT = 36 * 2**20
COLUMN_CUTS = (0, 2, 6, 11, 16)
TILE = 512


def attend(stack, bias_ref, own_ref, sib_ref, first_row, block_refs, out_ref):
    keys = jnp.concatenate([r[:, :HEAD] for r in block_refs], axis=0)
    values = jnp.concatenate([r[:, HEAD:] for r in block_refs], axis=0)
    values = jnp.concatenate([values, jnp.ones_like(values)], axis=1)
    scale = HEAD ** (-0.5) * LOG2E
    rows = out_ref.shape[0]
    heads = own_ref.shape[1] // HEAD
    at_rows = slice(first_row, first_row + rows)
    for side, q_ref in enumerate((own_ref, sib_ref)):
        for first in range(0, heads, stack):
            q = jnp.concatenate(
                [q_ref[at_rows, h * HEAD : (h + 1) * HEAD] for h in range(first, first + stack)],
                axis=0,
            )
            scores = lax.dot_general(
                q, keys, (((1,), (1,)), ((), ())), preferred_element_type=jnp.float32
            )
            mask = bias_ref[at_rows, :][None]
            scores = (scores.reshape(stack, rows, -1) + mask).reshape(scores.shape)
            top = jnp.max(scores, axis=1, keepdims=True)
            weights = jnp.exp2((scores - top) * scale).astype(jnp.bfloat16)
            mixed = jnp.dot(weights, values, preferred_element_type=jnp.float32)
            result = (mixed[:, :HEAD] / mixed[:, HEAD:]).astype(jnp.bfloat16)
            for i in range(stack):
                at = (side * heads + first + i) * HEAD
                out_ref[:, at : at + HEAD] = result[i * rows : (i + 1) * rows]


def weight_loads(first, own_w_ref, sib_w_ref, weight_ref, sems):
    half = own_w_ref.shape[0]
    tiles, _, tile = weight_ref.shape
    return [
        [
            pltpu.make_async_copy(
                ref.at[:, pl.ds(first + t * tile, tile)],
                weight_ref.at[t, pl.ds(i * half, half)],
                sems.at[t, i],
            )
            for i, ref in enumerate((own_w_ref, sib_w_ref))
        ]
        for t in range(tiles)
    ]


def project(first, attended_refs, weight_refs, out_refs, weight_ref, sems, beside=None):
    loads = weight_loads(first, *weight_refs, weight_ref, sems)
    for pair in loads:
        for load in pair:
            load.start()
    if beside:
        beside()
    tile = weight_ref.shape[2]
    for t, pair in enumerate(loads):
        for load in pair:
            load.wait()
        rows = jnp.concatenate([r[...] for r in attended_refs], axis=0)
        partial = jnp.dot(rows, weight_ref[t], preferred_element_type=jnp.float32)
        partial = partial.astype(jnp.bfloat16)
        at = 0
        for ref in out_refs:
            ref[:, pl.ds(t * tile, tile)] = partial[at : at + ref.shape[0]]
            at += ref.shape[0]


def prepare_kernel(offsets, positions_ref, queries_ref, own_w_ref, *refs):
    bias_ref, own_ref, swap_ref, weight_ref, sems = refs
    rows = queries_ref.shape[0]
    part = own_ref.shape[0] // 2
    run = rows // 2
    cp, tp = lax.axis_index("cp"), lax.axis_index("tp")
    side, core = tp // 2, tp % 2
    loads = [
        pltpu.make_async_copy(
            own_w_ref.at[:, pl.ds(0, weight_ref.shape[1])], weight_ref, sems.at[0]
        )
    ]
    for i, ref in enumerate((own_ref, swap_ref)):
        for half in range(2):
            row = ((side + half) % 2 * 2 + (core + i) % 2) * part
            loads.append(
                pltpu.make_async_copy(
                    queries_ref.at[pl.ds(row, part)],
                    ref.at[pl.ds(half * part, part)],
                    sems.at[1 + 2 * i + half],
                )
            )
    for load in loads[1:] + loads[:1]:
        load.start()
    lane = lax.broadcasted_iota(jnp.int32, (1, bias_ref.shape[1]), 1)
    key_pos = lane
    for j, (a, b) in enumerate(offsets):
        block = cp ^ jnp.where(core == 0, a, b)
        for half in range(2):
            at = j * rows + half * run
            start = positions_ref[block * rows + half * run]
            key_pos = jnp.where(lane >= at, lane + (start - at), key_pos)
    step = lax.broadcasted_iota(jnp.int32, (part, 1), 0)
    for half in range(2):
        token = ((side + half) % 2 * 2 + core) * part
        query_pos = positions_ref[cp * rows + token] + step
        bias_ref[pl.ds(half * part, part), :] = jnp.where(
            key_pos <= query_pos, 0.0, NEG
        ).astype(jnp.float32)
    for load in loads:
        load.wait()


def send_kernel(stack, bias_ref, own_ref, sib_ref, own_part_ref, sib_w_ref, *refs):
    block_refs = refs[:-4]
    attended_ref, out_ref, sib_part_ref, sems = refs[-4:]
    width = out_ref.shape[1]
    total = sib_part_ref.shape[1]
    loads = [
        pltpu.make_async_copy(sib_w_ref.at[:, cols], sib_part_ref.at[:, cols], sems.at[i])
        for i, cols in enumerate((pl.ds(0, width), pl.ds(width, total - width)))
    ]
    for load in loads:
        load.start()

    @pl.when(bias_ref[0, 0] <= 0.0)
    def _():
        row = attended_ref.shape[0]
        attend(stack, bias_ref, own_ref, sib_ref, row, block_refs, attended_ref)

    loads[0].wait()
    resident(pl.ds(0, width), attended_ref, own_part_ref, sib_part_ref, out_ref)
    loads[1].wait()


def resident(cols, attended_ref, own_part_ref, sib_part_ref, out_ref):
    half = own_part_ref.shape[0]
    partial = jnp.dot(
        attended_ref[:, :half], own_part_ref[:, cols], preferred_element_type=jnp.float32
    ) + jnp.dot(attended_ref[:, half:], sib_part_ref[:, cols], preferred_element_type=jnp.float32)
    out_ref[...] = partial.astype(jnp.bfloat16)


def resident_kernel(first, attended_ref, own_part_ref, sib_part_ref, *out_refs):
    for ref in out_refs:
        cols = pl.ds(first, ref.shape[1])
        resident(cols, attended_ref, own_part_ref, sib_part_ref, ref)
        first += ref.shape[1]


def keep_kernel(stack, first, bias_ref, own_ref, sib_ref, own_w_ref, sib_w_ref, sent_ref, *refs):
    block_refs = refs[:-5]
    attended_ref, keep_ref, send_ref, weight_ref, sems = refs[-5:]

    def attention():
        @pl.when(bias_ref[0, 0] <= 0.0)
        def _():
            attend(stack, bias_ref, own_ref, sib_ref, 0, block_refs, attended_ref)

    project(
        first,
        (attended_ref, sent_ref),
        (own_w_ref, sib_w_ref),
        (keep_ref, send_ref),
        weight_ref,
        sems,
        attention,
    )


def project_kernel(first, own_w_ref, sib_w_ref, *refs):
    count = (len(refs) - 2) // 2
    project(
        first, refs[:count], (own_w_ref, sib_w_ref), refs[count:-2], refs[-2], refs[-1]
    )


def finish_kernel(first, *refs):
    keep_ref, got_ref = refs[:2]
    out_ref, sum_ref, sem = refs[-3:]
    sum_ref[...] = (
        keep_ref[...].astype(jnp.float32) + got_ref[...].astype(jnp.float32)
    ).astype(jnp.bfloat16)
    store = pltpu.make_async_copy(
        sum_ref, out_ref.at[:, pl.ds(first, sum_ref.shape[1])], sem
    )
    store.start()
    store.wait()


def pairing(cp_size):
    return [(o, o + 1) for o in range(cp_size - 2, 0, -2)]


def shards(cp_size, tp_size, queries, keys, values, positions, out_weight):
    rows = queries.shape[0]
    heads = queries.shape[1] // HEAD
    part = rows // tp_size
    tp = lax.axis_index("tp")

    def permute(x, to_cp, to_tp):
        pairs = [
            (c * tp_size + t, to_cp(c, t) * tp_size + to_tp(t))
            for c in range(cp_size)
            for t in range(tp_size)
        ]
        return lax.ppermute(x, AXES, pairs)

    def to_sibling(x):
        return permute(x, lambda c, t: c, lambda t: t ^ 1)

    kv_group = tp * heads // GROUP
    block = jnp.concatenate(
        [lax.dynamic_slice_in_dim(a, kv_group * HEAD, HEAD, 1) for a in (keys, values)], axis=1
    )
    blocks = [block]
    offsets = [(0, 0)]
    fetched = []
    for pair in pairing(cp_size):
        arrived = permute(block, lambda c, t, pair=pair: c ^ pair[t & 1], lambda t: t)
        fetched.append(arrived)
        blocks.append(arrived)
        offsets.append(pair)
    blocks.append(permute(block, lambda c, t: c ^ 1, lambda t: t))
    offsets.append((1, 1))
    for arrived, pair in zip(fetched, pairing(cp_size)):
        blocks.append(to_sibling(arrived))
        offsets.append((pair[1], pair[0]))

    width = out_weight.shape[1]
    cuts = [c * width // COLUMN_CUTS[-1] for c in COLUMN_CUTS]
    vmem = functools.partial(pltpu.with_memory_space_constraint, memory_space=pltpu.VMEM)
    sib_weight = to_sibling(out_weight)
    hbm = pl.BlockSpec(memory_space=pltpu.HBM)
    weights = [pltpu.with_memory_space_constraint(w, pltpu.HBM) for w in (out_weight, sib_weight)]
    whole = pl.BlockSpec(memory_space=pltpu.VMEM)
    token_count = positions.shape[0]
    stack = min(heads, max(1, 4 * 1536 // token_count))
    depth = 2 * heads * HEAD
    attended = pltpu.VMEM((part, depth), jnp.bfloat16)
    mine = (2 * part, heads * HEAD)
    bias, own_q, swap_q, own_part = pl.pallas_call(
        functools.partial(prepare_kernel, offsets),
        in_specs=[pl.BlockSpec(memory_space=pltpu.SMEM), hbm, hbm],
        out_shape=(
            pltpu.VMEM((2 * part, token_count), jnp.float32),
            pltpu.VMEM(mine, jnp.bfloat16),
            pltpu.VMEM(mine, jnp.bfloat16),
            pltpu.VMEM((heads * HEAD, cuts[2]), jnp.bfloat16),
        ),
        scratch_shapes=[pltpu.SemaphoreType.DMA((5,))],
        compiler_params=pltpu.CompilerParams(vmem_limit_bytes=VMEM_LIMIT),
        name="prepare",
    )(positions, pltpu.with_memory_space_constraint(queries, pltpu.HBM), weights[0])
    sib_q = to_sibling(swap_q)
    inputs = [vmem(bias), vmem(own_q), vmem(sib_q)]
    kv = [vmem(b) for b in blocks]

    def call(kernel, lo, hi, operands, in_specs, out_shape):
        return pl.pallas_call(
            kernel,
            in_specs=in_specs,
            out_shape=out_shape,
            scratch_shapes=[
                pltpu.VMEM(((hi - lo) // TILE, depth, TILE), jnp.bfloat16),
                pltpu.SemaphoreType.DMA(((hi - lo) // TILE, 2)),
            ],
            compiler_params=pltpu.CompilerParams(vmem_limit_bytes=VMEM_LIMIT),
        )(*operands)

    spans = list(zip(cuts[:-1], cuts[1:]))
    kept = [None] * len(spans)
    got = []
    for n, (lo, hi) in enumerate(spans):
        half = pltpu.VMEM((part, hi - lo), jnp.bfloat16)
        if n == 0:
            parts = pltpu.VMEM((depth // 2, cuts[2]), jnp.bfloat16)
            sent_rows, send, sib_part = pl.pallas_call(
                functools.partial(send_kernel, stack),
                in_specs=[whole] * 4 + [hbm] + [whole] * len(kv),
                out_shape=(attended, half, parts),
                scratch_shapes=[pltpu.SemaphoreType.DMA((2,))],
                compiler_params=pltpu.CompilerParams(vmem_limit_bytes=VMEM_LIMIT),
                name="send",
            )(*inputs, vmem(own_part), weights[1], *kv)
            parts = [vmem(own_part), vmem(sib_part)]
        elif n == 1:
            send = pl.pallas_call(
                functools.partial(resident_kernel, lo),
                in_specs=[whole] * 3,
                out_shape=half,
                compiler_params=pltpu.CompilerParams(vmem_limit_bytes=VMEM_LIMIT),
                name="again",
            )(vmem(sent_rows), *parts)
        elif n == 2:
            kept_rows, kept[n], send = call(
                functools.partial(keep_kernel, stack, lo),
                lo,
                hi,
                [*inputs, *weights, sent_rows, *kv],
                [whole] * 3 + [hbm] * 2 + [whole] * (1 + len(kv)),
                (attended, half, half),
            )
        else:
            kept[n], send = call(
                functools.partial(project_kernel, lo),
                lo,
                hi,
                [*weights, kept_rows, sent_rows],
                [hbm] * 2 + [whole] * 2,
                (half, half),
            )
        got.append(permute(send, lambda c, t: c, lambda t: t ^ 2))
    kept[:2] = pl.pallas_call(
        functools.partial(resident_kernel, 0),
        in_specs=[whole] * 3,
        out_shape=[pltpu.VMEM((part, hi - lo), jnp.bfloat16) for lo, hi in spans[:2]],
        compiler_params=pltpu.CompilerParams(vmem_limit_bytes=VMEM_LIMIT),
        name="rest",
    )(vmem(kept_rows), *parts)
    out = ()
    for lo, hi, keep, arrived in zip(cuts[:-1], cuts[1:], kept, got):
        out = pl.pallas_call(
            functools.partial(finish_kernel, lo),
            in_specs=[whole, whole] + [hbm] * len(out),
            out_specs=(hbm,),
            out_shape=(pltpu.HBM((part, width), jnp.bfloat16),),
            scratch_shapes=[pltpu.VMEM((part, hi - lo), jnp.bfloat16), pltpu.SemaphoreType.DMA],
            input_output_aliases={2: 0} if out else {},
            name="finish",
        )(vmem(keep), vmem(arrived), *out)
    return out[0]


def solution(mesh):
    in_specs = (P("cp", "tp"), P("cp", None), P("cp", None), P(), P("tp", None))
    out_specs = P(("cp", "tp"), None)
    cp_size, tp_size = mesh.shape["cp"], mesh.shape["tp"]

    def body(*args):
        return shards(cp_size, tp_size, *args)

    return jax.shard_map(body, mesh=mesh, in_specs=in_specs, out_specs=out_specs, check_vma=False)
```

```python
import functools

import jax
import jax.numpy as jnp
from jax import lax
from jax.experimental import pallas as pl
from jax.experimental.pallas import tpu as pltpu
from jax.sharding import PartitionSpec as P


HEAD = 128
GROUP = 8
NEG = -1e30
LOG2E = 1.4426950408889634
AXES = ("cp", "tp")
VMEM_LIMIT = 36 * 2**20
COLUMN_CUTS = (0, 2, 6, 11, 16)
TILE = 512


def attend(stack, bias_ref, own_ref, sib_ref, first_row, block_refs, out_ref):
    keys = jnp.concatenate([r[:, :HEAD] for r in block_refs], axis=0)
    values = jnp.concatenate([r[:, HEAD:] for r in block_refs], axis=0)
    values = jnp.concatenate([values, jnp.ones_like(values)], axis=1)
    scale = HEAD ** (-0.5) * LOG2E
    rows = out_ref.shape[0]
    heads = own_ref.shape[1] // HEAD
    at_rows = slice(first_row, first_row + rows)
    for side, q_ref in enumerate((own_ref, sib_ref)):
        for first in range(0, heads, stack):
            q = jnp.concatenate(
                [q_ref[at_rows, h * HEAD : (h + 1) * HEAD] for h in range(first, first + stack)],
                axis=0,
            )
            scores = lax.dot_general(
                q, keys, (((1,), (1,)), ((), ())), preferred_element_type=jnp.float32
            )
            mask = bias_ref[at_rows, :][None]
            scores = (scores.reshape(stack, rows, -1) + mask).reshape(scores.shape)
            top = jnp.max(scores, axis=1, keepdims=True)
            weights = jnp.exp2((scores - top) * scale).astype(jnp.bfloat16)
            mixed = jnp.dot(weights, values, preferred_element_type=jnp.float32)
            result = (mixed[:, :HEAD] / mixed[:, HEAD:]).astype(jnp.bfloat16)
            for i in range(stack):
                at = (side * heads + first + i) * HEAD
                out_ref[:, at : at + HEAD] = result[i * rows : (i + 1) * rows]


def weight_loads(first, own_w_ref, sib_w_ref, weight_ref, sems):
    half = own_w_ref.shape[0]
    tiles, _, tile = weight_ref.shape
    return [
        [
            pltpu.make_async_copy(
                ref.at[:, pl.ds(first + t * tile, tile)],
                weight_ref.at[t, pl.ds(i * half, half)],
                sems.at[t, i],
            )
            for i, ref in enumerate((own_w_ref, sib_w_ref))
        ]
        for t in range(tiles)
    ]


def project(first, attended_refs, weight_refs, out_refs, weight_ref, sems, beside=None):
    loads = weight_loads(first, *weight_refs, weight_ref, sems)
    for pair in loads:
        for load in pair:
            load.start()
    if beside:
        beside()
    tile = weight_ref.shape[2]
    for t, pair in enumerate(loads):
        for load in pair:
            load.wait()
        rows = jnp.concatenate([r[...] for r in attended_refs], axis=0)
        partial = jnp.dot(rows, weight_ref[t], preferred_element_type=jnp.float32)
        partial = partial.astype(jnp.bfloat16)
        at = 0
        for ref in out_refs:
            ref[:, pl.ds(t * tile, tile)] = partial[at : at + ref.shape[0]]
            at += ref.shape[0]


def prepare_kernel(offsets, positions_ref, queries_ref, own_w_ref, *refs):
    bias_ref, own_ref, swap_ref, weight_ref, sems = refs
    rows = queries_ref.shape[0]
    part = own_ref.shape[0] // 2
    run = rows // 2
    cp, tp = lax.axis_index("cp"), lax.axis_index("tp")
    side, core = tp // 2, tp % 2
    loads = [
        pltpu.make_async_copy(
            own_w_ref.at[:, pl.ds(0, weight_ref.shape[1])], weight_ref, sems.at[0]
        )
    ]
    for i, ref in enumerate((own_ref, swap_ref)):
        for half in range(2):
            row = ((side + half) % 2 * 2 + (core + i) % 2) * part
            loads.append(
                pltpu.make_async_copy(
                    queries_ref.at[pl.ds(row, part)],
                    ref.at[pl.ds(half * part, part)],
                    sems.at[1 + 2 * i + half],
                )
            )
    for load in loads[1:] + loads[:1]:
        load.start()
    lane = lax.broadcasted_iota(jnp.int32, (1, bias_ref.shape[1]), 1)
    key_pos = lane
    for j, (a, b) in enumerate(offsets):
        block = cp ^ jnp.where(core == 0, a, b)
        for half in range(2):
            at = j * rows + half * run
            start = positions_ref[block * rows + half * run]
            key_pos = jnp.where(lane >= at, lane + (start - at), key_pos)
    step = lax.broadcasted_iota(jnp.int32, (part, 1), 0)
    for half in range(2):
        token = ((side + half) % 2 * 2 + core) * part
        query_pos = positions_ref[cp * rows + token] + step
        bias_ref[pl.ds(half * part, part), :] = jnp.where(
            key_pos <= query_pos, 0.0, NEG
        ).astype(jnp.float32)
    for load in loads:
        load.wait()


def send_kernel(stack, bias_ref, own_ref, sib_ref, own_part_ref, sib_w_ref, *refs):
    block_refs = refs[:-4]
    attended_ref, out_ref, sib_part_ref, sems = refs[-4:]
    width = out_ref.shape[1]
    total = sib_part_ref.shape[1]
    loads = [
        pltpu.make_async_copy(sib_w_ref.at[:, cols], sib_part_ref.at[:, cols], sems.at[i])
        for i, cols in enumerate((pl.ds(0, width), pl.ds(width, total - width)))
    ]
    for load in loads:
        load.start()

    @pl.when(bias_ref[0, 0] <= 0.0)
    def _():
        row = attended_ref.shape[0]
        attend(stack, bias_ref, own_ref, sib_ref, row, block_refs, attended_ref)

    loads[0].wait()
    resident(pl.ds(0, width), attended_ref, own_part_ref, sib_part_ref, out_ref)
    loads[1].wait()


def resident(cols, attended_ref, own_part_ref, sib_part_ref, out_ref):
    half = own_part_ref.shape[0]
    partial = jnp.dot(
        attended_ref[:, :half], own_part_ref[:, cols], preferred_element_type=jnp.float32
    ) + jnp.dot(attended_ref[:, half:], sib_part_ref[:, cols], preferred_element_type=jnp.float32)
    out_ref[...] = partial.astype(jnp.bfloat16)


def resident_kernel(first, attended_ref, own_part_ref, sib_part_ref, *out_refs):
    for ref in out_refs:
        cols = pl.ds(first, ref.shape[1])
        resident(cols, attended_ref, own_part_ref, sib_part_ref, ref)
        first += ref.shape[1]


def keep_kernel(stack, first, bias_ref, own_ref, sib_ref, own_w_ref, sib_w_ref, sent_ref, *refs):
    block_refs = refs[:-5]
    attended_ref, keep_ref, send_ref, weight_ref, sems = refs[-5:]

    def attention():
        @pl.when(bias_ref[0, 0] <= 0.0)
        def _():
            attend(stack, bias_ref, own_ref, sib_ref, 0, block_refs, attended_ref)

    project(
        first,
        (attended_ref, sent_ref),
        (own_w_ref, sib_w_ref),
        (keep_ref, send_ref),
        weight_ref,
        sems,
        attention,
    )


def project_kernel(first, own_w_ref, sib_w_ref, *refs):
    count = (len(refs) - 2) // 2
    project(
        first, refs[:count], (own_w_ref, sib_w_ref), refs[count:-2], refs[-2], refs[-1]
    )


def finish_kernel(first, *refs):
    keep_ref, got_ref = refs[:2]
    out_ref, sum_ref, sem = refs[-3:]
    sum_ref[...] = (
        keep_ref[...].astype(jnp.float32) + got_ref[...].astype(jnp.float32)
    ).astype(jnp.bfloat16)
    store = pltpu.make_async_copy(
        sum_ref, out_ref.at[:, pl.ds(first, sum_ref.shape[1])], sem
    )
    store.start()
    store.wait()


def pairing(cp_size):
    half = cp_size // 2
    others = [o for o in range(2, cp_size, 2) if o != half]
    even = [half] + others
    odd = [half + 1] + [o + 1 for o in others[::-1]]
    return list(zip(even, odd))


def shards(cp_size, tp_size, queries, keys, values, positions, out_weight):
    rows = queries.shape[0]
    heads = queries.shape[1] // HEAD
    part = rows // tp_size
    tp = lax.axis_index("tp")

    def permute(x, to_cp, to_tp):
        pairs = [
            (c * tp_size + t, to_cp(c, t) * tp_size + to_tp(t))
            for c in range(cp_size)
            for t in range(tp_size)
        ]
        return lax.ppermute(x, AXES, pairs)

    def to_sibling(x):
        return permute(x, lambda c, t: c, lambda t: t ^ 1)

    kv_group = tp * heads // GROUP
    block = jnp.concatenate(
        [lax.dynamic_slice_in_dim(a, kv_group * HEAD, HEAD, 1) for a in (keys, values)], axis=1
    )
    blocks = [block]
    offsets = [(0, 0)]
    fetched = []
    for pair in pairing(cp_size):
        arrived = permute(block, lambda c, t, pair=pair: c ^ pair[t & 1], lambda t: t)
        fetched.append(arrived)
        blocks.append(arrived)
        offsets.append(pair)
    blocks.append(permute(block, lambda c, t: c ^ 1, lambda t: t))
    offsets.append((1, 1))
    for arrived, pair in zip(fetched, pairing(cp_size)):
        blocks.append(to_sibling(arrived))
        offsets.append((pair[1], pair[0]))

    width = out_weight.shape[1]
    cuts = [c * width // COLUMN_CUTS[-1] for c in COLUMN_CUTS]
    vmem = functools.partial(pltpu.with_memory_space_constraint, memory_space=pltpu.VMEM)
    sib_weight = to_sibling(out_weight)
    hbm = pl.BlockSpec(memory_space=pltpu.HBM)
    weights = [pltpu.with_memory_space_constraint(w, pltpu.HBM) for w in (out_weight, sib_weight)]
    whole = pl.BlockSpec(memory_space=pltpu.VMEM)
    token_count = positions.shape[0]
    stack = min(heads, max(1, 4 * 1536 // token_count))
    depth = 2 * heads * HEAD
    attended = pltpu.VMEM((part, depth), jnp.bfloat16)
    mine = (2 * part, heads * HEAD)
    bias, own_q, swap_q, own_part = pl.pallas_call(
        functools.partial(prepare_kernel, offsets),
        in_specs=[pl.BlockSpec(memory_space=pltpu.SMEM), hbm, hbm],
        out_shape=(
            pltpu.VMEM((2 * part, token_count), jnp.float32),
            pltpu.VMEM(mine, jnp.bfloat16),
            pltpu.VMEM(mine, jnp.bfloat16),
            pltpu.VMEM((heads * HEAD, cuts[2]), jnp.bfloat16),
        ),
        scratch_shapes=[pltpu.SemaphoreType.DMA((5,))],
        compiler_params=pltpu.CompilerParams(vmem_limit_bytes=VMEM_LIMIT),
        name="prepare",
    )(positions, pltpu.with_memory_space_constraint(queries, pltpu.HBM), weights[0])
    sib_q = to_sibling(swap_q)
    inputs = [vmem(bias), vmem(own_q), vmem(sib_q)]
    kv = [vmem(b) for b in blocks]

    def call(kernel, lo, hi, operands, in_specs, out_shape):
        return pl.pallas_call(
            kernel,
            in_specs=in_specs,
            out_shape=out_shape,
            scratch_shapes=[
                pltpu.VMEM(((hi - lo) // TILE, depth, TILE), jnp.bfloat16),
                pltpu.SemaphoreType.DMA(((hi - lo) // TILE, 2)),
            ],
            compiler_params=pltpu.CompilerParams(vmem_limit_bytes=VMEM_LIMIT),
        )(*operands)

    spans = list(zip(cuts[:-1], cuts[1:]))
    kept = [None] * len(spans)
    got = []
    for n, (lo, hi) in enumerate(spans):
        half = pltpu.VMEM((part, hi - lo), jnp.bfloat16)
        if n == 0:
            parts = pltpu.VMEM((depth // 2, cuts[2]), jnp.bfloat16)
            sent_rows, send, sib_part = pl.pallas_call(
                functools.partial(send_kernel, stack),
                in_specs=[whole] * 4 + [hbm] + [whole] * len(kv),
                out_shape=(attended, half, parts),
                scratch_shapes=[pltpu.SemaphoreType.DMA((2,))],
                compiler_params=pltpu.CompilerParams(vmem_limit_bytes=VMEM_LIMIT),
                name="send",
            )(*inputs, vmem(own_part), weights[1], *kv)
            parts = [vmem(own_part), vmem(sib_part)]
        elif n == 1:
            send = pl.pallas_call(
                functools.partial(resident_kernel, lo),
                in_specs=[whole] * 3,
                out_shape=half,
                compiler_params=pltpu.CompilerParams(vmem_limit_bytes=VMEM_LIMIT),
                name="again",
            )(vmem(sent_rows), *parts)
        elif n == 2:
            kept_rows, kept[n], send = call(
                functools.partial(keep_kernel, stack, lo),
                lo,
                hi,
                [*inputs, *weights, sent_rows, *kv],
                [whole] * 3 + [hbm] * 2 + [whole] * (1 + len(kv)),
                (attended, half, half),
            )
        else:
            kept[n], send = call(
                functools.partial(project_kernel, lo),
                lo,
                hi,
                [*weights, kept_rows, sent_rows],
                [hbm] * 2 + [whole] * 2,
                (half, half),
            )
        got.append(permute(send, lambda c, t: c, lambda t: t ^ 2))
    kept[:2] = pl.pallas_call(
        functools.partial(resident_kernel, 0),
        in_specs=[whole] * 3,
        out_shape=[pltpu.VMEM((part, hi - lo), jnp.bfloat16) for lo, hi in spans[:2]],
        compiler_params=pltpu.CompilerParams(vmem_limit_bytes=VMEM_LIMIT),
        name="rest",
    )(vmem(kept_rows), *parts)
    out = ()
    for lo, hi, keep, arrived in zip(cuts[:-1], cuts[1:], kept, got):
        out = pl.pallas_call(
            functools.partial(finish_kernel, lo),
            in_specs=[whole, whole] + [hbm] * len(out),
            out_specs=(hbm,),
            out_shape=(pltpu.HBM((part, width), jnp.bfloat16),),
            scratch_shapes=[pltpu.VMEM((part, hi - lo), jnp.bfloat16), pltpu.SemaphoreType.DMA],
            input_output_aliases={2: 0} if out else {},
            name="finish",
        )(vmem(keep), vmem(arrived), *out)
    return out[0]


def solution(mesh):
    in_specs = (P("cp", "tp"), P("cp", None), P("cp", None), P(), P("tp", None))
    out_specs = P(("cp", "tp"), None)
    cp_size, tp_size = mesh.shape["cp"], mesh.shape["tp"]

    def body(*args):
        return shards(cp_size, tp_size, *args)

    return jax.shard_map(body, mesh=mesh, in_specs=in_specs, out_specs=out_specs, check_vma=False)
```

```python
import functools

import jax
import jax.numpy as jnp
from jax import lax
from jax.experimental import pallas as pl
from jax.experimental.pallas import tpu as pltpu
from jax.sharding import PartitionSpec as P


HEAD = 128
GROUP = 8
NEG = -1e30
LOG2E = 1.4426950408889634
AXES = ("cp", "tp")
VMEM_LIMIT = 36 * 2**20
COLUMN_CUTS = (0, 2, 5, 9, 13, 16)
TILE = 512


def attend(stack, bias_ref, own_ref, sib_ref, first_row, block_refs, out_ref):
    keys = jnp.concatenate([r[:, :HEAD] for r in block_refs], axis=0)
    values = jnp.concatenate([r[:, HEAD:] for r in block_refs], axis=0)
    values = jnp.concatenate([values, jnp.ones_like(values)], axis=1)
    scale = HEAD ** (-0.5) * LOG2E
    rows = out_ref.shape[0]
    heads = own_ref.shape[1] // HEAD
    at_rows = slice(first_row, first_row + rows)
    groups = [(side, first) for side in range(2) for first in range(0, heads, stack)]

    def scores_of(side, first):
        q_ref = (own_ref, sib_ref)[side]
        q = jnp.concatenate(
            [q_ref[at_rows, h * HEAD : (h + 1) * HEAD] for h in range(first, first + stack)],
            axis=0,
        )
        return lax.dot_general(
            q, keys, (((1,), (1,)), ((), ())), preferred_element_type=jnp.float32
        )

    ahead = [scores_of(*group) for group in groups[:2]]
    for n, (side, first) in enumerate(groups):
        mask = bias_ref[at_rows, :][None]
        scores = ahead.pop(0)
        scores = (scores.reshape(stack, rows, -1) + mask).reshape(scores.shape)
        top = jnp.max(scores, axis=1, keepdims=True)
        weights = jnp.exp2((scores - top) * scale).astype(jnp.bfloat16)
        if n + 2 < len(groups):
            ahead.append(scores_of(*groups[n + 2]))
        mixed = jnp.dot(weights, values, preferred_element_type=jnp.float32)
        result = (mixed[:, :HEAD] / mixed[:, HEAD:]).astype(jnp.bfloat16)
        for i in range(stack):
            at = (side * heads + first + i) * HEAD
            out_ref[:, at : at + HEAD] = result[i * rows : (i + 1) * rows]


def weight_loads(first, own_w_ref, sib_w_ref, weight_ref, sems):
    half = own_w_ref.shape[0]
    tiles, _, tile = weight_ref.shape
    return [
        [
            pltpu.make_async_copy(
                ref.at[:, pl.ds(first + t * tile, tile)],
                weight_ref.at[t, pl.ds(i * half, half)],
                sems.at[t, i],
            )
            for i, ref in enumerate((own_w_ref, sib_w_ref))
        ]
        for t in range(tiles)
    ]


def project(first, attended_refs, weight_refs, out_refs, weight_ref, sems, beside=None):
    loads = weight_loads(first, *weight_refs, weight_ref, sems)
    for pair in loads:
        for load in pair:
            load.start()
    if beside:
        beside()
    tile = weight_ref.shape[2]
    for t, pair in enumerate(loads):
        for load in pair:
            load.wait()
        rows = jnp.concatenate([r[...] for r in attended_refs], axis=0)
        partial = jnp.dot(rows, weight_ref[t], preferred_element_type=jnp.float32)
        partial = partial.astype(jnp.bfloat16)
        at = 0
        for ref in out_refs:
            ref[:, pl.ds(t * tile, tile)] = partial[at : at + ref.shape[0]]
            at += ref.shape[0]


def prepare_kernel(offsets, positions_ref, queries_ref, own_w_ref, *refs):
    bias_ref, own_ref, swap_ref, weight_ref, sems = refs
    rows = queries_ref.shape[0]
    part = own_ref.shape[0] // 2
    run = rows // 2
    cp, tp = lax.axis_index("cp"), lax.axis_index("tp")
    side, core = tp // 2, tp % 2
    loads = [
        pltpu.make_async_copy(
            own_w_ref.at[:, pl.ds(0, weight_ref.shape[1])], weight_ref, sems.at[0]
        )
    ]
    for i, ref in enumerate((own_ref, swap_ref)):
        for half in range(2):
            row = ((side + half) % 2 * 2 + (core + i) % 2) * part
            loads.append(
                pltpu.make_async_copy(
                    queries_ref.at[pl.ds(row, part)],
                    ref.at[pl.ds(half * part, part)],
                    sems.at[1 + 2 * i + half],
                )
            )
    for load in loads[1:] + loads[:1]:
        load.start()
    lane = lax.broadcasted_iota(jnp.int32, (1, bias_ref.shape[1]), 1)
    key_pos = lane
    for j, (a, b) in enumerate(offsets):
        block = cp ^ jnp.where(core == 0, a, b)
        for half in range(2):
            at = j * rows + half * run
            start = positions_ref[block * rows + half * run]
            key_pos = jnp.where(lane >= at, lane + (start - at), key_pos)
    step = lax.broadcasted_iota(jnp.int32, (part, 1), 0)
    for half in range(2):
        token = ((side + half) % 2 * 2 + core) * part
        query_pos = positions_ref[cp * rows + token] + step
        bias_ref[pl.ds(half * part, part), :] = jnp.where(
            key_pos <= query_pos, 0.0, NEG
        ).astype(jnp.float32)
    for load in loads:
        load.wait()


def send_kernel(stack, bias_ref, own_ref, sib_ref, own_part_ref, sib_w_ref, *refs):
    block_refs = refs[:-4]
    attended_ref, out_ref, sib_part_ref, sems = refs[-4:]
    width = out_ref.shape[1]
    total = sib_part_ref.shape[1]
    loads = [
        pltpu.make_async_copy(sib_w_ref.at[:, cols], sib_part_ref.at[:, cols], sems.at[i])
        for i, cols in enumerate((pl.ds(0, width), pl.ds(width, total - width)))
    ]
    for load in loads:
        load.start()

    @pl.when(bias_ref[0, 0] <= 0.0)
    def _():
        row = attended_ref.shape[0]
        attend(stack, bias_ref, own_ref, sib_ref, row, block_refs, attended_ref)

    loads[0].wait()
    resident(pl.ds(0, width), attended_ref, own_part_ref, sib_part_ref, out_ref)
    loads[1].wait()


def resident(cols, attended_ref, own_part_ref, sib_part_ref, out_ref):
    half = own_part_ref.shape[0]
    partial = jnp.dot(
        attended_ref[:, :half], own_part_ref[:, cols], preferred_element_type=jnp.float32
    ) + jnp.dot(attended_ref[:, half:], sib_part_ref[:, cols], preferred_element_type=jnp.float32)
    out_ref[...] = partial.astype(jnp.bfloat16)


def resident_kernel(first, attended_ref, own_part_ref, sib_part_ref, *out_refs):
    for ref in out_refs:
        cols = pl.ds(first, ref.shape[1])
        resident(cols, attended_ref, own_part_ref, sib_part_ref, ref)
        first += ref.shape[1]


def keep_kernel(stack, first, bias_ref, own_ref, sib_ref, own_w_ref, sib_w_ref, sent_ref, *refs):
    block_refs = refs[:-5]
    attended_ref, keep_ref, send_ref, weight_ref, sems = refs[-5:]

    def attention():
        @pl.when(bias_ref[0, 0] <= 0.0)
        def _():
            attend(stack, bias_ref, own_ref, sib_ref, 0, block_refs, attended_ref)

    project(
        first,
        (attended_ref, sent_ref),
        (own_w_ref, sib_w_ref),
        (keep_ref, send_ref),
        weight_ref,
        sems,
        attention,
    )


def project_kernel(first, own_w_ref, sib_w_ref, *refs):
    count = (len(refs) - 2) // 2
    project(
        first, refs[:count], (own_w_ref, sib_w_ref), refs[count:-2], refs[-2], refs[-1]
    )


def finish_kernel(first, *refs):
    keep_ref, got_ref = refs[:2]
    out_ref, sum_ref, sem = refs[-3:]
    sum_ref[...] = (
        keep_ref[...].astype(jnp.float32) + got_ref[...].astype(jnp.float32)
    ).astype(jnp.bfloat16)
    store = pltpu.make_async_copy(
        sum_ref, out_ref.at[:, pl.ds(first, sum_ref.shape[1])], sem
    )
    store.start()
    store.wait()


def pairing(cp_size):
    half = cp_size // 2
    others = [o for o in range(2, cp_size, 2) if o != half]
    even = [half] + others
    odd = [half + 1] + [o + 1 for o in others[::-1]]
    return list(zip(even, odd))


def shards(cp_size, tp_size, queries, keys, values, positions, out_weight):
    rows = queries.shape[0]
    heads = queries.shape[1] // HEAD
    part = rows // tp_size
    tp = lax.axis_index("tp")

    def permute(x, to_cp, to_tp):
        pairs = [
            (c * tp_size + t, to_cp(c, t) * tp_size + to_tp(t))
            for c in range(cp_size)
            for t in range(tp_size)
        ]
        return lax.ppermute(x, AXES, pairs)

    def to_sibling(x):
        return permute(x, lambda c, t: c, lambda t: t ^ 1)

    kv_group = tp * heads // GROUP
    block = jnp.concatenate(
        [lax.dynamic_slice_in_dim(a, kv_group * HEAD, HEAD, 1) for a in (keys, values)], axis=1
    )
    blocks = [block]
    offsets = [(0, 0)]
    fetched = []
    for pair in pairing(cp_size):
        arrived = permute(block, lambda c, t, pair=pair: c ^ pair[t & 1], lambda t: t)
        fetched.append(arrived)
        blocks.append(arrived)
        offsets.append(pair)
    blocks.append(permute(block, lambda c, t: c ^ 1, lambda t: t))
    offsets.append((1, 1))
    for arrived, pair in zip(fetched, pairing(cp_size)):
        blocks.append(to_sibling(arrived))
        offsets.append((pair[1], pair[0]))

    width = out_weight.shape[1]
    cuts = [c * width // COLUMN_CUTS[-1] for c in COLUMN_CUTS]
    vmem = functools.partial(pltpu.with_memory_space_constraint, memory_space=pltpu.VMEM)
    sib_weight = to_sibling(out_weight)
    hbm = pl.BlockSpec(memory_space=pltpu.HBM)
    weights = [pltpu.with_memory_space_constraint(w, pltpu.HBM) for w in (out_weight, sib_weight)]
    whole = pl.BlockSpec(memory_space=pltpu.VMEM)
    token_count = positions.shape[0]
    stack = min(heads, max(1, 4 * 1536 // token_count))
    depth = 2 * heads * HEAD
    attended = pltpu.VMEM((part, depth), jnp.bfloat16)
    mine = (2 * part, heads * HEAD)
    bias, own_q, swap_q, own_part = pl.pallas_call(
        functools.partial(prepare_kernel, offsets),
        in_specs=[pl.BlockSpec(memory_space=pltpu.SMEM), hbm, hbm],
        out_shape=(
            pltpu.VMEM((2 * part, token_count), jnp.float32),
            pltpu.VMEM(mine, jnp.bfloat16),
            pltpu.VMEM(mine, jnp.bfloat16),
            pltpu.VMEM((heads * HEAD, cuts[2]), jnp.bfloat16),
        ),
        scratch_shapes=[pltpu.SemaphoreType.DMA((5,))],
        compiler_params=pltpu.CompilerParams(vmem_limit_bytes=VMEM_LIMIT),
        name="prepare",
    )(positions, pltpu.with_memory_space_constraint(queries, pltpu.HBM), weights[0])
    sib_q = to_sibling(swap_q)
    inputs = [vmem(bias), vmem(own_q), vmem(sib_q)]
    kv = [vmem(b) for b in blocks]

    def call(kernel, lo, hi, operands, in_specs, out_shape):
        return pl.pallas_call(
            kernel,
            in_specs=in_specs,
            out_shape=out_shape,
            scratch_shapes=[
                pltpu.VMEM(((hi - lo) // TILE, depth, TILE), jnp.bfloat16),
                pltpu.SemaphoreType.DMA(((hi - lo) // TILE, 2)),
            ],
            compiler_params=pltpu.CompilerParams(vmem_limit_bytes=VMEM_LIMIT),
        )(*operands)

    spans = list(zip(cuts[:-1], cuts[1:]))
    kept = [None] * len(spans)
    got = []
    for n, (lo, hi) in enumerate(spans):
        half = pltpu.VMEM((part, hi - lo), jnp.bfloat16)
        if n == 0:
            parts = pltpu.VMEM((depth // 2, cuts[2]), jnp.bfloat16)
            sent_rows, send, sib_part = pl.pallas_call(
                functools.partial(send_kernel, stack),
                in_specs=[whole] * 4 + [hbm] + [whole] * len(kv),
                out_shape=(attended, half, parts),
                scratch_shapes=[pltpu.SemaphoreType.DMA((2,))],
                compiler_params=pltpu.CompilerParams(vmem_limit_bytes=VMEM_LIMIT),
                name="send",
            )(*inputs, vmem(own_part), weights[1], *kv)
            parts = [vmem(own_part), vmem(sib_part)]
        elif n == 1:
            send = pl.pallas_call(
                functools.partial(resident_kernel, lo),
                in_specs=[whole] * 3,
                out_shape=half,
                compiler_params=pltpu.CompilerParams(vmem_limit_bytes=VMEM_LIMIT),
                name="again",
            )(vmem(sent_rows), *parts)
        elif n == 2:
            kept_rows, kept[n], send = call(
                functools.partial(keep_kernel, stack, lo),
                lo,
                hi,
                [*inputs, *weights, sent_rows, *kv],
                [whole] * 3 + [hbm] * 2 + [whole] * (1 + len(kv)),
                (attended, half, half),
            )
        else:
            kept[n], send = call(
                functools.partial(project_kernel, lo),
                lo,
                hi,
                [*weights, kept_rows, sent_rows],
                [hbm] * 2 + [whole] * 2,
                (half, half),
            )
        got.append(permute(send, lambda c, t: c, lambda t: t ^ 2))
    kept[:2] = pl.pallas_call(
        functools.partial(resident_kernel, 0),
        in_specs=[whole] * 3,
        out_shape=[pltpu.VMEM((part, hi - lo), jnp.bfloat16) for lo, hi in spans[:2]],
        compiler_params=pltpu.CompilerParams(vmem_limit_bytes=VMEM_LIMIT),
        name="rest",
    )(vmem(kept_rows), *parts)
    out = ()
    for lo, hi, keep, arrived in zip(cuts[:-1], cuts[1:], kept, got):
        out = pl.pallas_call(
            functools.partial(finish_kernel, lo),
            in_specs=[whole, whole] + [hbm] * len(out),
            out_specs=(hbm,),
            out_shape=(pltpu.HBM((part, width), jnp.bfloat16),),
            scratch_shapes=[pltpu.VMEM((part, hi - lo), jnp.bfloat16), pltpu.SemaphoreType.DMA],
            input_output_aliases={2: 0} if out else {},
            name="finish",
        )(vmem(keep), vmem(arrived), *out)
    return out[0]


def solution(mesh):
    in_specs = (P("cp", "tp"), P("cp", None), P("cp", None), P(), P("tp", None))
    out_specs = P(("cp", "tp"), None)
    cp_size, tp_size = mesh.shape["cp"], mesh.shape["tp"]

    def body(*args):
        return shards(cp_size, tp_size, *args)

    return jax.shard_map(body, mesh=mesh, in_specs=in_specs, out_specs=out_specs, check_vma=False)
```

```python
import functools

import jax
import jax.numpy as jnp
from jax import lax
from jax.experimental import pallas as pl
from jax.experimental.pallas import tpu as pltpu
from jax.sharding import PartitionSpec as P


HEAD = 128
GROUP = 8
NEG = -1e30
LOG2E = 1.4426950408889634
AXES = ("cp", "tp")
VMEM_LIMIT = 36 * 2**20
COLUMN_CUTS = (0, 2, 5, 9, 13, 16)
TILE = 512


def attend(stack, bias_ref, own_ref, sib_ref, first_row, block_refs, out_ref):
    keys = jnp.concatenate([r[:, :HEAD] for r in block_refs], axis=0)
    values = jnp.concatenate([r[:, HEAD:] for r in block_refs], axis=0)
    values = jnp.concatenate([values, jnp.ones_like(values)], axis=1)
    scale = HEAD ** (-0.5) * LOG2E
    rows = out_ref.shape[0]
    heads = own_ref.shape[1] // HEAD
    at_rows = slice(first_row, first_row + rows)
    groups = [(side, first) for side in range(2) for first in range(0, heads, stack)]

    def scores_of(side, first):
        q_ref = (own_ref, sib_ref)[side]
        q = jnp.concatenate(
            [q_ref[at_rows, h * HEAD : (h + 1) * HEAD] for h in range(first, first + stack)],
            axis=0,
        )
        return lax.dot_general(
            q, keys, (((1,), (1,)), ((), ())), preferred_element_type=jnp.float32
        )

    ahead = [scores_of(*group) for group in groups[:2]]
    for n, (side, first) in enumerate(groups):
        mask = bias_ref[at_rows, :][None]
        scores = ahead.pop(0)
        scores = (scores.reshape(stack, rows, -1) + mask).reshape(scores.shape)
        top = jnp.max(scores, axis=1, keepdims=True)
        weights = jnp.exp2((scores - top) * scale).astype(jnp.bfloat16)
        if n + 2 < len(groups):
            ahead.append(scores_of(*groups[n + 2]))
        mixed = jnp.dot(weights, values, preferred_element_type=jnp.float32)
        result = (mixed[:, :HEAD] / mixed[:, HEAD:]).astype(jnp.bfloat16)
        for i in range(stack):
            at = (side * heads + first + i) * HEAD
            out_ref[:, at : at + HEAD] = result[i * rows : (i + 1) * rows]


def weight_loads(first, own_w_ref, sib_w_ref, weight_ref, sems):
    half = own_w_ref.shape[0]
    tiles, _, tile = weight_ref.shape
    return [
        [
            pltpu.make_async_copy(
                ref.at[:, pl.ds(first + t * tile, tile)],
                weight_ref.at[t, pl.ds(i * half, half)],
                sems.at[t, i],
            )
            for i, ref in enumerate((own_w_ref, sib_w_ref))
        ]
        for t in range(tiles)
    ]


def project(first, attended_refs, weight_refs, out_refs, weight_ref, sems, beside=None):
    loads = weight_loads(first, *weight_refs, weight_ref, sems)
    for pair in loads:
        for load in pair:
            load.start()
    if beside:
        beside()
    tile = weight_ref.shape[2]
    for t, pair in enumerate(loads):
        for load in pair:
            load.wait()
        rows = jnp.concatenate([r[...] for r in attended_refs], axis=0)
        partial = jnp.dot(rows, weight_ref[t], preferred_element_type=jnp.float32)
        partial = partial.astype(jnp.bfloat16)
        at = 0
        for ref in out_refs:
            ref[:, pl.ds(t * tile, tile)] = partial[at : at + ref.shape[0]]
            at += ref.shape[0]


def prepare_kernel(offsets, all_positions_ref, queries_ref, own_w_ref, *refs):
    bias_ref, own_ref, swap_ref, weight_ref, positions_ref, sems = refs
    positions_load = pltpu.make_async_copy(all_positions_ref, positions_ref, sems.at[5])
    positions_load.start()
    rows = queries_ref.shape[0]
    part = own_ref.shape[0] // 2
    run = rows // 2
    cp, tp = lax.axis_index("cp"), lax.axis_index("tp")
    side, core = tp // 2, tp % 2
    loads = [
        pltpu.make_async_copy(
            own_w_ref.at[:, pl.ds(0, weight_ref.shape[1])], weight_ref, sems.at[0]
        )
    ]
    for i, ref in enumerate((own_ref, swap_ref)):
        for half in range(2):
            row = ((side + half) % 2 * 2 + (core + i) % 2) * part
            loads.append(
                pltpu.make_async_copy(
                    queries_ref.at[pl.ds(row, part)],
                    ref.at[pl.ds(half * part, part)],
                    sems.at[1 + 2 * i + half],
                )
            )
    for load in loads[1:] + loads[:1]:
        load.start()
    positions_load.wait()
    lane = lax.broadcasted_iota(jnp.int32, (1, bias_ref.shape[1]), 1)
    key_pos = lane
    for j, (a, b) in enumerate(offsets):
        block = cp ^ jnp.where(core == 0, a, b)
        for half in range(2):
            at = j * rows + half * run
            start = positions_ref[block * rows + half * run]
            key_pos = jnp.where(lane >= at, lane + (start - at), key_pos)
    step = lax.broadcasted_iota(jnp.int32, (part, 1), 0)
    for half in range(2):
        token = ((side + half) % 2 * 2 + core) * part
        query_pos = positions_ref[cp * rows + token] + step
        bias_ref[pl.ds(half * part, part), :] = jnp.where(
            key_pos <= query_pos, 0.0, NEG
        ).astype(jnp.float32)
    for load in loads:
        load.wait()


def send_kernel(stack, bias_ref, own_ref, sib_ref, own_part_ref, sib_w_ref, *refs):
    block_refs = refs[:-4]
    attended_ref, out_ref, sib_part_ref, sems = refs[-4:]
    width = out_ref.shape[1]
    total = sib_part_ref.shape[1]
    loads = [
        pltpu.make_async_copy(sib_w_ref.at[:, cols], sib_part_ref.at[:, cols], sems.at[i])
        for i, cols in enumerate((pl.ds(0, width), pl.ds(width, total - width)))
    ]
    for load in loads:
        load.start()

    @pl.when(bias_ref[0, 0] <= 0.0)
    def _():
        row = attended_ref.shape[0]
        attend(stack, bias_ref, own_ref, sib_ref, row, block_refs, attended_ref)

    loads[0].wait()
    resident(pl.ds(0, width), attended_ref, own_part_ref, sib_part_ref, out_ref)
    loads[1].wait()


def resident(cols, attended_ref, own_part_ref, sib_part_ref, out_ref):
    half = own_part_ref.shape[0]
    partial = jnp.dot(
        attended_ref[:, :half], own_part_ref[:, cols], preferred_element_type=jnp.float32
    ) + jnp.dot(attended_ref[:, half:], sib_part_ref[:, cols], preferred_element_type=jnp.float32)
    out_ref[...] = partial.astype(jnp.bfloat16)


def resident_kernel(first, attended_ref, own_part_ref, sib_part_ref, *out_refs):
    for ref in out_refs:
        cols = pl.ds(first, ref.shape[1])
        resident(cols, attended_ref, own_part_ref, sib_part_ref, ref)
        first += ref.shape[1]


def keep_kernel(stack, first, bias_ref, own_ref, sib_ref, own_w_ref, sib_w_ref, sent_ref, *refs):
    block_refs = refs[:-5]
    attended_ref, keep_ref, send_ref, weight_ref, sems = refs[-5:]

    def attention():
        @pl.when(bias_ref[0, 0] <= 0.0)
        def _():
            attend(stack, bias_ref, own_ref, sib_ref, 0, block_refs, attended_ref)

    project(
        first,
        (attended_ref, sent_ref),
        (own_w_ref, sib_w_ref),
        (keep_ref, send_ref),
        weight_ref,
        sems,
        attention,
    )


def project_kernel(first, own_w_ref, sib_w_ref, *refs):
    count = (len(refs) - 2) // 2
    project(
        first, refs[:count], (own_w_ref, sib_w_ref), refs[count:-2], refs[-2], refs[-1]
    )


def finish_kernel(first, *refs):
    keep_ref, got_ref = refs[:2]
    out_ref, sum_ref, sem = refs[-3:]
    sum_ref[...] = (
        keep_ref[...].astype(jnp.float32) + got_ref[...].astype(jnp.float32)
    ).astype(jnp.bfloat16)
    store = pltpu.make_async_copy(
        sum_ref, out_ref.at[:, pl.ds(first, sum_ref.shape[1])], sem
    )
    store.start()
    store.wait()


def pairing(cp_size):
    half = cp_size // 2
    others = [o for o in range(2, cp_size, 2) if o != half]
    even = [half] + others
    odd = [half + 1] + [o + 1 for o in others[::-1]]
    return list(zip(even, odd))


def shards(cp_size, tp_size, queries, keys, values, positions, out_weight):
    rows = queries.shape[0]
    heads = queries.shape[1] // HEAD
    part = rows // tp_size
    tp = lax.axis_index("tp")

    def permute(x, to_cp, to_tp):
        pairs = [
            (c * tp_size + t, to_cp(c, t) * tp_size + to_tp(t))
            for c in range(cp_size)
            for t in range(tp_size)
        ]
        return lax.ppermute(x, AXES, pairs)

    def to_sibling(x):
        return permute(x, lambda c, t: c, lambda t: t ^ 1)

    kv_group = tp * heads // GROUP
    block = jnp.concatenate(
        [lax.dynamic_slice_in_dim(a, kv_group * HEAD, HEAD, 1) for a in (keys, values)], axis=1
    )
    blocks = [block]
    offsets = [(0, 0)]
    fetched = []
    for pair in pairing(cp_size):
        arrived = permute(block, lambda c, t, pair=pair: c ^ pair[t & 1], lambda t: t)
        fetched.append(arrived)
        blocks.append(arrived)
        offsets.append(pair)
    blocks.append(permute(block, lambda c, t: c ^ 1, lambda t: t))
    offsets.append((1, 1))
    for arrived, pair in zip(fetched, pairing(cp_size)):
        blocks.append(to_sibling(arrived))
        offsets.append((pair[1], pair[0]))

    width = out_weight.shape[1]
    cuts = [c * width // COLUMN_CUTS[-1] for c in COLUMN_CUTS]
    vmem = functools.partial(pltpu.with_memory_space_constraint, memory_space=pltpu.VMEM)
    sib_weight = to_sibling(out_weight)
    hbm = pl.BlockSpec(memory_space=pltpu.HBM)
    weights = [pltpu.with_memory_space_constraint(w, pltpu.HBM) for w in (out_weight, sib_weight)]
    whole = pl.BlockSpec(memory_space=pltpu.VMEM)
    token_count = positions.shape[0]
    stack = min(heads, max(1, 4 * 1536 // token_count))
    depth = 2 * heads * HEAD
    attended = pltpu.VMEM((part, depth), jnp.bfloat16)
    mine = (2 * part, heads * HEAD)
    bias, own_q, swap_q, own_part = pl.pallas_call(
        functools.partial(prepare_kernel, offsets),
        in_specs=[hbm, hbm, hbm],
        out_shape=(
            pltpu.VMEM((2 * part, token_count), jnp.float32),
            pltpu.VMEM(mine, jnp.bfloat16),
            pltpu.VMEM(mine, jnp.bfloat16),
            pltpu.VMEM((heads * HEAD, cuts[2]), jnp.bfloat16),
        ),
        scratch_shapes=[
            pltpu.SMEM((token_count,), jnp.int32),
            pltpu.SemaphoreType.DMA((6,)),
        ],
        compiler_params=pltpu.CompilerParams(vmem_limit_bytes=VMEM_LIMIT),
        name="prepare",
    )(*[pltpu.with_memory_space_constraint(x, pltpu.HBM) for x in (positions, queries)], weights[0])
    sib_q = to_sibling(swap_q)
    inputs = [vmem(bias), vmem(own_q), vmem(sib_q)]
    kv = [vmem(b) for b in blocks]

    def call(kernel, lo, hi, operands, in_specs, out_shape):
        return pl.pallas_call(
            kernel,
            in_specs=in_specs,
            out_shape=out_shape,
            scratch_shapes=[
                pltpu.VMEM(((hi - lo) // TILE, depth, TILE), jnp.bfloat16),
                pltpu.SemaphoreType.DMA(((hi - lo) // TILE, 2)),
            ],
            compiler_params=pltpu.CompilerParams(vmem_limit_bytes=VMEM_LIMIT),
        )(*operands)

    spans = list(zip(cuts[:-1], cuts[1:]))
    kept = [None] * len(spans)
    got = []
    for n, (lo, hi) in enumerate(spans):
        half = pltpu.VMEM((part, hi - lo), jnp.bfloat16)
        if n == 0:
            parts = pltpu.VMEM((depth // 2, cuts[2]), jnp.bfloat16)
            sent_rows, send, sib_part = pl.pallas_call(
                functools.partial(send_kernel, stack),
                in_specs=[whole] * 4 + [hbm] + [whole] * len(kv),
                out_shape=(attended, half, parts),
                scratch_shapes=[pltpu.SemaphoreType.DMA((2,))],
                compiler_params=pltpu.CompilerParams(vmem_limit_bytes=VMEM_LIMIT),
                name="send",
            )(*inputs, vmem(own_part), weights[1], *kv)
            parts = [vmem(own_part), vmem(sib_part)]
        elif n == 1:
            send = pl.pallas_call(
                functools.partial(resident_kernel, lo),
                in_specs=[whole] * 3,
                out_shape=half,
                compiler_params=pltpu.CompilerParams(vmem_limit_bytes=VMEM_LIMIT),
                name="again",
            )(vmem(sent_rows), *parts)
        elif n == 2:
            kept_rows, kept[n], send = call(
                functools.partial(keep_kernel, stack, lo),
                lo,
                hi,
                [*inputs, *weights, sent_rows, *kv],
                [whole] * 3 + [hbm] * 2 + [whole] * (1 + len(kv)),
                (attended, half, half),
            )
        else:
            kept[n], send = call(
                functools.partial(project_kernel, lo),
                lo,
                hi,
                [*weights, kept_rows, sent_rows],
                [hbm] * 2 + [whole] * 2,
                (half, half),
            )
        got.append(permute(send, lambda c, t: c, lambda t: t ^ 2))
    kept[:2] = pl.pallas_call(
        functools.partial(resident_kernel, 0),
        in_specs=[whole] * 3,
        out_shape=[pltpu.VMEM((part, hi - lo), jnp.bfloat16) for lo, hi in spans[:2]],
        compiler_params=pltpu.CompilerParams(vmem_limit_bytes=VMEM_LIMIT),
        name="rest",
    )(vmem(kept_rows), *parts)
    out = ()
    for lo, hi, keep, arrived in zip(cuts[:-1], cuts[1:], kept, got):
        out = pl.pallas_call(
            functools.partial(finish_kernel, lo),
            in_specs=[whole, whole] + [hbm] * len(out),
            out_specs=(hbm,),
            out_shape=(pltpu.HBM((part, width), jnp.bfloat16),),
            scratch_shapes=[pltpu.VMEM((part, hi - lo), jnp.bfloat16), pltpu.SemaphoreType.DMA],
            input_output_aliases={2: 0} if out else {},
            name="finish",
        )(vmem(keep), vmem(arrived), *out)
    return out[0]


def solution(mesh):
    in_specs = (P("cp", "tp"), P("cp", None), P("cp", None), P(), P("tp", None))
    out_specs = P(("cp", "tp"), None)
    cp_size, tp_size = mesh.shape["cp"], mesh.shape["tp"]

    def body(*args):
        return shards(cp_size, tp_size, *args)

    return jax.shard_map(body, mesh=mesh, in_specs=in_specs, out_specs=out_specs, check_vma=False)
```
